32 devices in a mesh: shard: 4 (over z), ctx: 4 (over y, x), tp: 2 (over core).
Axes of the slice: x: 2, y: 2, z: 4, core: 2. Of those that a mesh axis runs over, the one named last changes fastest.
Arguments:
- hidden_in: bfloat16 [4, 512, 1536], P('shard', 'ctx'), may hold values from -6 to 6
- seg_start: int32 [4, 512], P('shard', 'ctx'), may hold values from 0 to 511, as said below
- norm1_gain: bfloat16 [1536], P('shard'), may hold values from 0.5 to 1.5
- w_qkv: bfloat16 [1536, 2, 8, 128], P('shard', 'tp'), may hold values from -0.15625 to 0.15625
- b_qkv: bfloat16 [128, 2, 8], P('shard', 'tp'), may hold values from -2 to 2
- w_attn_out: bfloat16 [1536, 1536], P('shard', 'tp'), may hold values from -0.875 to 0.875
- norm2_gain: bfloat16 [1536], P('shard'), may hold values from 0.5 to 1.5
- w_gate_up: bfloat16 [1536, 2, 8960], P('shard', None, 'tp'), may hold values from -0.15625 to 0.15625
- w_down: bfloat16 [1536, 8960], P('shard', 'tp'), may hold values from -0.0625 to 0.0625
- out_grad: bfloat16 [4, 512, 1536], P('shard', 'ctx'), may hold values from -6 to 6
Outputs:
- layer_out: float32 [4, 512, 1536], P('shard', 'ctx')
- in_grad: float32 [4, 512, 1536], P('shard', 'ctx')
- grad_norm1: float32 [1536], P('shard')
- grad_qkv: float32 [1536, 2, 8, 128], P('shard', 'tp')
- grad_bias: float32 [128, 2, 8], P('shard', 'tp')
- grad_attn_out: float32 [1536, 1536], P('shard', 'tp')
- grad_norm2: float32 [1536], P('shard')
- grad_gate_up: float32 [1536, 2, 8960], P('shard', None, 'tp')
- grad_down: float32 [1536, 8960], P('shard', 'tp')
The draws below stay inside these ranges and needn't reach their ends.
Inputs may be any that keep to these rules, and one draw needn't show every extreme that they name: seg_start never falls along a row and equals its own position at a segment's first token; every segment holds 1 to 256 tokens, and every row has a segment of exactly 256 tokens.
All inputs are finite; a program needn't handle non-finite values.
Results may differ from the reference program's by a relative error of at most 0.02.
Values may be sent and summed in bfloat16 or wider, within the bound.
A program may use at most 320 MiB of HBM per device.

```python
import jax
import jax.numpy as jnp
from jax import lax

D = 1536
H = 12
KV = 2
HD = 128
FF = 8960
TOK_DEV = 128
SLOTS = 8
ROWS = 4
LEN = 512
SEG_MAX = 256


def draw_seg_start(key, part):
    flag_key, begin_key = jax.random.split(jax.random.fold_in(key, 11))
    flags = jax.random.randint(flag_key, (ROWS, LEN), 0, max(SEG_MAX // 4, 2)) == 0
    begin = jax.random.randint(begin_key, (ROWS, 1), 0, LEN - SEG_MAX + 1)
    positions = jnp.arange(LEN, dtype=jnp.int32)[None, :]
    inside = (positions > begin) & (positions < begin + SEG_MAX)
    flags = flags & jnp.logical_not(inside) | (positions == begin) | (positions == begin + SEG_MAX) | (positions == 0)

    def advance(current, column):
        flag_col, position = column
        renewed = jnp.where(flag_col | (position - current >= SEG_MAX), position, current)
        return (renewed, renewed)
    unused, starts = lax.scan(advance, jnp.zeros((ROWS,), jnp.int32), (flags.T, jnp.arange(LEN, dtype=jnp.int32)))
    return starts.T.astype(jnp.int32)


def level_of(stream_key, shape, cuts, smallest, top_value):
    def one(dim, blocks):
        heights = jax.random.uniform(jax.random.fold_in(jax.random.fold_in(stream_key, 6), dim), (blocks,), jnp.float32, smallest / len(cuts), top_value / len(cuts))
        return jnp.repeat(jnp.exp(heights), shape[dim] // blocks).reshape((-1,) + (1,) * (len(shape) - dim - 1))

    level = one(*cuts[0])
    for cut in cuts[1:]:
        level = level * one(*cut)
    return level


def centred(key, dims, deviation, reach, shards=(), held_as=jnp.bfloat16):
    values = deviation * jax.random.normal(key, dims, jnp.float32)
    if shards:
        values = values * level_of(key, dims, shards, -0.22, 0.18)
    return jnp.clip(values, -reach, reach).astype(held_as)


def setup_inputs(seed: int = 0) -> dict:
    splits = jax.random.split(jax.random.key(seed), 11)
    hidden_in = centred(splits[0], (ROWS, LEN, D), 1.0, 6.0, ((0, 4), (1, 4)))
    seg_start = draw_seg_start(jax.random.fold_in(splits[10], 71), 0)
    norm1_gain = jnp.clip(1.0 + 0.1 * jax.random.normal(splits[2], (D,), jnp.float32), 0.5, 1.5).astype(jnp.bfloat16)
    w_qkv = centred(splits[3], (D, KV, SLOTS, HD), D ** -0.5, 0.15625, ((0, 4), (1, 2)))
    b_qkv = centred(splits[4], (HD, KV, SLOTS), 0.5, 2.0, ((0, 4), (1, 2)))
    w_attn_out = centred(splits[5], (D, H * HD), (8 * H * HD // SEG_MAX) ** -0.5, 0.875, ((0, 4), (1, 2)))
    norm2_gain = jnp.clip(1.0 + 0.1 * jax.random.normal(splits[6], (D,), jnp.float32), 0.5, 1.5).astype(jnp.bfloat16)
    w_gate_up = centred(splits[7], (D, 2, FF), D ** -0.5, 0.15625, ((0, 4), (2, 2)))
    w_down = centred(splits[8], (D, FF), FF ** -0.5, 0.0625, ((0, 4), (1, 2)))
    out_grad = centred(splits[9], (ROWS, LEN, D), 1.0, 6.0, ((0, 4), (1, 4)))
    return dict(hidden_in=hidden_in, seg_start=seg_start, norm1_gain=norm1_gain, w_qkv=w_qkv, b_qkv=b_qkv, w_attn_out=w_attn_out, norm2_gain=norm2_gain, w_gate_up=w_gate_up, w_down=w_down, out_grad=out_grad)


EPSILON = 1e-06
ROPE_BASE = 1000000.0

def rope_tables(positions, head_dim):
    half_dim = head_dim // 2
    frequency = ROPE_BASE ** (-(jnp.arange(half_dim, dtype=jnp.float32) * 2.0) / head_dim)
    angles = positions[:, None] * frequency[None, :]
    cosine = jnp.cos(angles)
    sine_vals = jnp.sin(angles)
    return (jnp.concatenate([cosine, cosine], -1), jnp.concatenate([sine_vals, sine_vals], -1))

def rotate_half(values):
    half_dim = values.shape[-1] // 2
    return jnp.concatenate([-values[..., half_dim:], values[..., :half_dim]], -1)

def rotate_back(values):
    half_dim = values.shape[-1] // 2
    return jnp.concatenate([values[..., half_dim:], -values[..., :half_dim]], -1)

def apply_rope(values, cosine, sine_vals):
    return values * cosine + rotate_half(values) * sine_vals

def rope_grad(grads, cosine, sine_vals):
    return grads * cosine + rotate_back(grads * sine_vals)

def rms_back(grad_norm, inputs, inv_rms, gain_vals):
    scaled = gain_vals * grad_norm
    return inv_rms * scaled - inputs * (inv_rms * inv_rms * inv_rms) * lax.optimization_barrier(jnp.mean(scaled * inputs, -1, keepdims=True))

def reference(hidden_in, seg_start, norm1_gain, w_qkv, b_qkv, w_attn_out, norm2_gain, w_gate_up, w_down, out_grad):
    gain_one = norm1_gain.astype(jnp.float32)
    gain_two = norm2_gain.astype(jnp.float32)
    qkv_weight = w_qkv.astype(jnp.float32)
    gate_up_weight = w_gate_up.astype(jnp.float32)
    bias_vals = jnp.transpose(b_qkv.astype(jnp.float32), (1, 2, 0))
    groups = H // KV
    query_scale = HD ** (-0.5)
    block_count = LEN // TOK_DEV
    token_ids = jnp.arange(LEN, dtype=jnp.int32)
    highest = lax.Precision.HIGHEST

    def block_mask(first_row, seg_row):
        query_ids = first_row + jnp.arange(TOK_DEV, dtype=jnp.int32)
        seg_block = lax.dynamic_slice_in_dim(seg_row, first_row, TOK_DEV, 0)
        return (token_ids[None, :] <= query_ids[:, None]) & (token_ids[None, :] >= seg_block[:, None])

    def one_row(totals, row_inputs):
        row_x, seg_row, row_grad = row_inputs
        inputs = row_x.astype(jnp.float32)
        inv_rms1 = lax.rsqrt(lax.optimization_barrier(jnp.mean(inputs * inputs, -1, keepdims=True)) + EPSILON)
        normed1 = (inputs * inv_rms1 * gain_one).astype(jnp.bfloat16)
        qkv_vals = jnp.einsum('td,dcsh->tcsh', normed1.astype(jnp.float32), qkv_weight) + bias_vals
        cosine, sine_vals = rope_tables((token_ids - seg_row).astype(jnp.float32), HD)
        cos_four = cosine[:, None, None, :]
        sin_four = sine_vals[:, None, None, :]
        cos_three = cosine[:, None, :]
        sin_three = sine_vals[:, None, :]
        q_rot = (apply_rope(qkv_vals[:, :, :groups], cos_four, sin_four) * query_scale).astype(jnp.bfloat16)
        k_rot = apply_rope(qkv_vals[:, :, groups], cos_three, sin_three).astype(jnp.bfloat16)
        v_vals = qkv_vals[:, :, groups + 1].astype(jnp.bfloat16)
        key_float = k_rot.astype(jnp.float32)
        value_float = v_vals.astype(jnp.float32)

        def forward_block(block_no):
            first_row = block_no * TOK_DEV
            allowed = block_mask(first_row, seg_row)
            q_block = lax.dynamic_slice_in_dim(q_rot, first_row, TOK_DEV, 0).astype(jnp.float32)
            scores = jnp.einsum('qcgh,kch->cgqk', q_block, key_float)
            scores = jnp.where(allowed, scores, -jnp.inf)
            top_vals = lax.optimization_barrier(jnp.max(scores, -1))
            log_total = top_vals + jnp.log(lax.optimization_barrier(jnp.sum(jnp.exp(scores - top_vals[..., None]), -1)))
            attn_probs = jnp.where(allowed, jnp.exp(scores - log_total[..., None]), 0.0)
            outputs = jnp.einsum('cgqk,kch->qcgh', attn_probs, value_float, precision=highest)
            return (outputs, log_total)
        attn_blocks, lse_blocks = lax.map(forward_block, jnp.arange(block_count, dtype=jnp.int32))
        attn_bf = attn_blocks.reshape(LEN, KV, groups, HD).astype(jnp.bfloat16)
        attn_flat = attn_bf.reshape(LEN, H * HD)
        resid1 = inputs + jnp.dot(attn_flat, w_attn_out.T, preferred_element_type=jnp.float32)
        inv_rms2 = lax.rsqrt(lax.optimization_barrier(jnp.mean(resid1 * resid1, -1, keepdims=True)) + EPSILON)
        normed2 = (resid1 * inv_rms2 * gain_two).astype(jnp.bfloat16)
        gate_up = jnp.einsum('td,dsf->tsf', normed2.astype(jnp.float32), gate_up_weight)
        gate_vals = gate_up[:, 0]
        up_vals = gate_up[:, 1]
        sigmoid_gate = jax.nn.sigmoid(gate_vals)
        silu_gate = gate_vals * sigmoid_gate
        hidden_act = (silu_gate * up_vals).astype(jnp.bfloat16)
        layer_row = resid1 + jnp.dot(hidden_act, w_down.T, preferred_element_type=jnp.float32)
        d_hidden = jnp.dot(row_grad, w_down, preferred_element_type=jnp.float32)
        grad_down = jnp.dot(row_grad.T, hidden_act, preferred_element_type=jnp.float32)
        d_gate = d_hidden * up_vals * sigmoid_gate * (1.0 + gate_vals * (1.0 - sigmoid_gate))
        d_up = d_hidden * silu_gate
        d_gate_up = jnp.stack([d_gate, d_up], 1).astype(jnp.bfloat16)
        grad_gate_up = jnp.einsum('td,tsf->dsf', normed2.astype(jnp.float32), d_gate_up.astype(jnp.float32))
        d_normed2 = jnp.einsum('tsf,dsf->td', d_gate_up.astype(jnp.float32), gate_up_weight)
        grad_norm2 = lax.optimization_barrier(jnp.sum(d_normed2 * resid1 * inv_rms2, 0))
        d_resid1 = row_grad.astype(jnp.float32) + rms_back(d_normed2, resid1, inv_rms2, gain_two)
        d_resid1_bf = d_resid1.astype(jnp.bfloat16)
        d_attn = jnp.dot(d_resid1_bf, w_attn_out, preferred_element_type=jnp.float32).reshape(LEN, KV, groups, HD)
        grad_attn_out = jnp.dot(d_resid1_bf.T, attn_flat, preferred_element_type=jnp.float32)

        def backward_block(sums, block_no):
            first_row = block_no * TOK_DEV
            allowed = block_mask(first_row, seg_row)
            q_block = lax.dynamic_slice_in_dim(q_rot, first_row, TOK_DEV, 0).astype(jnp.float32)
            out_block = lax.dynamic_slice_in_dim(attn_bf, first_row, TOK_DEV, 0).astype(jnp.float32)
            grad_block = lax.dynamic_slice_in_dim(d_attn, first_row, TOK_DEV, 0)
            grad_bf = grad_block.astype(jnp.bfloat16).astype(jnp.float32)
            delta_vals = jnp.transpose(lax.optimization_barrier(jnp.sum(grad_block * out_block, -1)), (1, 2, 0))
            scores = jnp.einsum('qcgh,kch->cgqk', q_block, key_float)
            attn_probs = jnp.where(allowed, jnp.exp(scores - lse_blocks[block_no][..., None]), 0.0)
            probs_bf = attn_probs.astype(jnp.bfloat16).astype(jnp.float32)
            d_value = jnp.einsum('cgqk,qcgh->kch', probs_bf, grad_bf)
            d_probs = jnp.einsum('qcgh,kch->cgqk', grad_bf, value_float)
            d_scores = (attn_probs * (d_probs - delta_vals[..., None])).astype(jnp.bfloat16).astype(jnp.float32)
            d_query = jnp.einsum('cgqk,kch->qcgh', d_scores, key_float)
            d_key = jnp.einsum('cgqk,qcgh->kch', d_scores, q_block)
            return ((sums[0] + d_key, sums[1] + d_value), d_query)
        zero_keys = jnp.zeros((LEN, KV, HD), jnp.float32)
        key_sums, d_query_blocks = lax.scan(backward_block, (zero_keys, zero_keys), jnp.arange(block_count, dtype=jnp.int32))
        d_query = d_query_blocks.reshape(LEN, KV, groups, HD)
        d_qkv = jnp.concatenate([rope_grad(d_query, cos_four, sin_four) * query_scale, rope_grad(key_sums[0], cos_three, sin_three)[:, :, None], key_sums[1][:, :, None]], 2)
        grad_bias = jnp.transpose(lax.optimization_barrier(jnp.sum(d_qkv, 0)), (2, 0, 1))
        d_qkv_bf = d_qkv.astype(jnp.bfloat16).astype(jnp.float32)
        grad_qkv = jnp.einsum('td,tcsh->dcsh', normed1.astype(jnp.float32), d_qkv_bf)
        d_normed1 = jnp.einsum('tcsh,dcsh->td', d_qkv_bf, qkv_weight)
        grad_norm1 = lax.optimization_barrier(jnp.sum(d_normed1 * inputs * inv_rms1, 0))
        in_row = d_resid1 + rms_back(d_normed1, inputs, inv_rms1, gain_one)
        new_totals = (totals[0] + grad_norm1, totals[1] + grad_qkv, totals[2] + grad_bias, totals[3] + grad_attn_out, totals[4] + grad_norm2, totals[5] + grad_gate_up, totals[6] + grad_down)
        return (new_totals, (layer_row, in_row))
    start_totals = (jnp.zeros((D,), jnp.float32), jnp.zeros((D, KV, H // KV + 2, HD), jnp.float32), jnp.zeros((HD, KV, H // KV + 2), jnp.float32), jnp.zeros((D, H * HD), jnp.float32), jnp.zeros((D,), jnp.float32), jnp.zeros((D, 2, FF), jnp.float32), jnp.zeros((D, FF), jnp.float32))
    totals, row_outs = lax.scan(one_row, start_totals, (hidden_in, seg_start, out_grad))
    grad_scale = float(ROWS * LEN) ** (-0.5)
    return (row_outs[0], row_outs[1], totals[0] * grad_scale, totals[1] * grad_scale, totals[2] * grad_scale, totals[3] * grad_scale, totals[4] * grad_scale, totals[5] * grad_scale, totals[6] * grad_scale)
```

```python
import jax
import jax.numpy as jnp
from jax import lax
from jax.sharding import PartitionSpec as P

EPSILON = 1e-06
ROPE_BASE = 1000000.0
NEGATIVE = -1e30


def rope_tables(positions, head_dim):
    half_dim = head_dim // 2
    frequency = ROPE_BASE ** (-(jnp.arange(half_dim, dtype=jnp.float32) * 2.0) / head_dim)
    angles = positions[:, None] * frequency[None, :]
    cosine = jnp.cos(angles)
    sine_vals = jnp.sin(angles)
    return (jnp.concatenate([cosine, cosine], -1), jnp.concatenate([sine_vals, sine_vals], -1))


def rotate_half(values):
    half_dim = values.shape[-1] // 2
    return jnp.concatenate([-values[..., half_dim:], values[..., :half_dim]], -1)


def rotate_back(values):
    half_dim = values.shape[-1] // 2
    return jnp.concatenate([values[..., half_dim:], -values[..., :half_dim]], -1)


def apply_rope(values, cosine, sine_vals):
    return values * cosine + rotate_half(values) * sine_vals


def rope_grad(grads, cosine, sine_vals):
    return grads * cosine + rotate_back(grads * sine_vals)


def rms_back(grad_norm, inputs, inv_rms, gain_vals):
    scaled = gain_vals * grad_norm
    return inv_rms * scaled - inputs * (inv_rms * inv_rms * inv_rms) * jnp.mean(
        scaled * inputs, -1, keepdims=True
    )


def tensor_sum(partial_sum):
    return lax.psum(partial_sum, "tp")


def contract_rows(left, right):
    return lax.dot_general(
        left, right, (((0,), (0,)), ((), ())), preferred_element_type=jnp.float32
    )


def contract_cols(left, right):
    return lax.dot_general(
        left, right, (((1,), (1,)), ((), ())), preferred_element_type=jnp.float32
    )

def body(
    hidden_in,
    seg_start,
    norm1_gain,
    w_qkv,
    b_qkv,
    w_attn_out,
    norm2_gain,
    w_gate_up,
    w_down,
    out_grad,
):
    shards = lax.axis_size("shard")
    ctxs = lax.axis_size("ctx")
    ctx_id = lax.axis_index("ctx")
    tp_id = lax.axis_index("tp")
    everyone = ("shard", "ctx", "tp")
    bf16 = jnp.bfloat16
    qkv_full, attn_out_full, gain_one_bf, bias_full, gain_two_bf = (
        lax.all_gather(w_qkv, "shard", axis=0, tiled=True),
        lax.all_gather(w_attn_out, "shard", axis=0, tiled=True),
        lax.all_gather(norm1_gain, "shard", axis=0, tiled=True),
        lax.all_gather(b_qkv, "shard", axis=0, tiled=True),
        lax.all_gather(norm2_gain, "shard", axis=0, tiled=True),
    )
    tokens, width = hidden_in.shape[1], hidden_in.shape[2]
    half = tokens // lax.axis_size("tp")
    part = w_gate_up.shape[0]
    hidden_units = w_down.shape[1] // (shards * ctxs)

    def my_units(weights):
        blocks = weights.reshape(weights.shape[:-1] + (ctxs, shards * hidden_units))
        return lax.dynamic_index_in_dim(blocks, ctx_id, weights.ndim - 1, keepdims=False)

    def my_half(rows):
        return lax.dynamic_slice_in_dim(rows, tp_id * half, half, 0)

    mine = jnp.concatenate([my_units(w_gate_up), my_units(w_down)[:, None]], 1)
    mine = jnp.transpose(mine.reshape(part, 3, shards, hidden_units), (2, 0, 1, 3))
    units = lax.all_to_all(mine, "shard", split_axis=0, concat_axis=0, tiled=True)
    units = units.reshape(shards * part, 3, hidden_units)
    gate_up_w = units[:, :2].reshape(shards * part, 2 * hidden_units)
    down_w = units[:, 2]
    grad_rows = out_grad[0]
    grad_all = lax.all_gather(my_half(grad_rows), everyone, axis=0, tiled=True)

    kv_local = qkv_full.shape[1]
    head_dim = qkv_full.shape[3]
    groups = qkv_full.shape[2] - 2
    query_scale = head_dim ** (-0.5)
    grad_scale = float(shards * ctxs * tokens) ** (-0.5)
    gain_one = gain_one_bf.astype(jnp.float32)
    gain_two = gain_two_bf.astype(jnp.float32)
    bias_vals = jnp.transpose(bias_full.astype(jnp.float32), (1, 2, 0))
    inputs = hidden_in[0].astype(jnp.float32)
    seg_row = seg_start[0]
    token_ids = ctx_id * tokens + jnp.arange(tokens, dtype=jnp.int32)
    cosine, sine_vals = rope_tables((token_ids - seg_row).astype(jnp.float32), head_dim)
    cos_four = cosine[:, None, None, :]
    sin_four = sine_vals[:, None, None, :]
    cos_three = cosine[:, None, :]
    sin_three = sine_vals[:, None, :]
    inv_rms1 = lax.rsqrt(jnp.mean(inputs * inputs, -1, keepdims=True) + EPSILON)
    normed1 = (inputs * inv_rms1 * gain_one).astype(bf16)
    qkv_vals = (
        jnp.einsum("td,dcsh->tcsh", normed1, qkv_full, preferred_element_type=jnp.float32)
        + bias_vals
    )
    q_rot = (apply_rope(qkv_vals[:, :, :groups], cos_four, sin_four) * query_scale).astype(bf16)
    k_rot = apply_rope(qkv_vals[:, :, groups], cos_three, sin_three).astype(bf16)
    v_vals = qkv_vals[:, :, groups + 1].astype(bf16)
    query_heads = jnp.transpose(q_rot, (1, 2, 0, 3))
    key_value = jnp.stack([k_rot, v_vals], axis=2)
    key_value = lax.all_gather(key_value, "ctx", axis=0, tiled=True)
    keys, values = key_value[:, :, 0], key_value[:, :, 1]
    length = keys.shape[0]
    key_ids = jnp.arange(length, dtype=jnp.int32)
    allowed = (key_ids[None, :] <= token_ids[:, None]) & (key_ids[None, :] >= seg_row[:, None])
    scores = jnp.einsum("cgqh,kch->cgqk", query_heads, keys, preferred_element_type=jnp.float32)
    scores = jnp.where(allowed, scores, NEGATIVE)
    top_all = jnp.max(scores, -1, keepdims=True)
    raised = jnp.where(allowed, jnp.exp(scores - top_all), 0.0)
    total_all = jnp.sum(raised, -1, keepdims=True)
    attn_probs = raised / total_all
    probs_bf = attn_probs.astype(bf16)
    attn_vals = jnp.einsum(
        "cgqk,kch->cgqh", probs_bf, values, preferred_element_type=jnp.float32
    ).astype(bf16)
    attn_flat = jnp.transpose(attn_vals, (2, 0, 1, 3)).reshape(tokens, kv_local * groups * head_dim)
    resid1 = inputs + tensor_sum(contract_cols(attn_flat, attn_out_full))
    inv_rms2 = lax.rsqrt(jnp.mean(resid1 * resid1, -1, keepdims=True) + EPSILON)
    normed2 = (resid1 * inv_rms2 * gain_two).astype(bf16)

    normed2_all = lax.all_gather(my_half(normed2), everyone, axis=0, tiled=True)
    gate_up = jnp.dot(normed2_all, gate_up_w, preferred_element_type=jnp.float32)
    gate_vals, up_vals = gate_up[:, :hidden_units], gate_up[:, hidden_units:]
    sigmoid_gate = jax.nn.sigmoid(gate_vals)
    silu_gate = gate_vals * sigmoid_gate
    hidden_act = (silu_gate * up_vals).astype(bf16)
    d_hidden = jnp.dot(grad_all, down_w, preferred_element_type=jnp.float32)
    d_gate = d_hidden * up_vals * sigmoid_gate * (1.0 + gate_vals * (1.0 - sigmoid_gate))
    d_up = d_hidden * silu_gate
    d_gate_up = jnp.concatenate([d_gate, d_up], 1).astype(bf16)

    def scatter_sum(partial_sum):
        share = lax.psum_scatter(
            partial_sum.astype(bf16), everyone, scatter_dimension=0, tiled=True
        )
        return lax.all_gather(share, "tp", axis=0, tiled=True).astype(jnp.float32)

    d_normed2 = scatter_sum(contract_cols(d_gate_up, gate_up_w))
    layer_out = resid1 + scatter_sum(contract_cols(hidden_act, down_w))
    grad_down = contract_rows(grad_all, hidden_act).astype(bf16)
    grad_gate_up = contract_rows(normed2_all, d_gate_up).astype(bf16)
    made = jnp.concatenate([grad_gate_up, grad_down], 1).reshape(shards, part, 3 * hidden_units)
    made = lax.all_to_all(made, "shard", split_axis=0, concat_axis=0, tiled=True)
    made = lax.all_gather(made, "ctx", axis=0, tiled=False)
    made = made.reshape(ctxs, shards, part, 3, hidden_units)
    made = jnp.transpose(made, (2, 3, 0, 1, 4)).reshape(part, 3, ctxs * shards * hidden_units)
    made = made.astype(jnp.float32) * grad_scale

    grad_norm2 = jnp.sum(d_normed2 * resid1 * inv_rms2, 0)
    d_resid1 = grad_rows.astype(jnp.float32) + rms_back(d_normed2, resid1, inv_rms2, gain_two)
    d_resid1_bf = d_resid1.astype(bf16)
    d_attn_flat = jnp.dot(d_resid1_bf, attn_out_full, preferred_element_type=jnp.float32)
    grad_attn_out = contract_rows(d_resid1_bf, attn_flat)
    d_attn = jnp.transpose(d_attn_flat.reshape(tokens, kv_local, groups, head_dim), (1, 2, 0, 3))
    delta_vals = jnp.sum(d_attn * attn_vals.astype(jnp.float32), -1)
    d_attn_bf = d_attn.astype(bf16)
    d_value = jnp.einsum("cgqk,cgqh->kch", probs_bf, d_attn_bf, preferred_element_type=jnp.float32)
    d_probs = jnp.einsum("cgqh,kch->cgqk", d_attn_bf, values, preferred_element_type=jnp.float32)
    d_scores = (attn_probs * (d_probs - delta_vals[..., None])).astype(bf16)
    d_query = jnp.einsum("cgqk,kch->cgqh", d_scores, keys, preferred_element_type=jnp.float32)
    d_key = jnp.einsum("cgqk,cgqh->kch", d_scores, query_heads, preferred_element_type=jnp.float32)
    key_grads = lax.psum_scatter(
        jnp.stack([d_key, d_value], 2).astype(bf16), "ctx", scatter_dimension=0, tiled=True
    ).astype(jnp.float32)
    d_query_rows = jnp.transpose(d_query, (2, 0, 1, 3))
    d_qkv = jnp.concatenate(
        [
            rope_grad(d_query_rows, cos_four, sin_four) * query_scale,
            rope_grad(key_grads[:, :, 0], cos_three, sin_three)[:, :, None],
            key_grads[:, :, 1][:, :, None],
        ],
        2,
    )
    grad_bias = jnp.transpose(jnp.sum(d_qkv, 0), (2, 0, 1))
    d_qkv_bf = d_qkv.astype(bf16)
    grad_qkv = jnp.einsum("td,tcsh->dcsh", normed1, d_qkv_bf, preferred_element_type=jnp.float32)
    d_normed1 = tensor_sum(
        jnp.einsum("tcsh,dcsh->td", d_qkv_bf, qkv_full, preferred_element_type=jnp.float32)
    )
    grad_norm1 = jnp.sum(d_normed1 * inputs * inv_rms1, 0)
    in_grad = d_resid1 + rms_back(d_normed1, inputs, inv_rms1, gain_one)

    def total(partial_sum):
        share = lax.psum_scatter(
            partial_sum.astype(bf16), "shard", scatter_dimension=0, tiled=True
        )
        return lax.psum(share, "ctx").astype(jnp.float32) * grad_scale

    return (
        layer_out[None],
        in_grad[None],
        total(grad_norm1),
        total(grad_qkv),
        total(grad_bias),
        total(grad_attn_out),
        total(grad_norm2),
        made[:, :2],
        made[:, 2],
    )


def solution(mesh):
    in_specs = (
        P("shard", "ctx", None),
        P("shard", "ctx"),
        P("shard"),
        P("shard", "tp", None, None),
        P("shard", "tp", None),
        P("shard", "tp"),
        P("shard"),
        P("shard", None, "tp"),
        P("shard", "tp"),
        P("shard", "ctx", None),
    )
    out_specs = (
        P("shard", "ctx", None),
        P("shard", "ctx", None),
        P("shard"),
        P("shard", "tp", None, None),
        P("shard", "tp", None),
        P("shard", "tp"),
        P("shard"),
        P("shard", None, "tp"),
        P("shard", "tp"),
    )
    return jax.shard_map(body, mesh=mesh, in_specs=in_specs, out_specs=out_specs, check_vma=False)
```
